128 devices in a mesh: left: 16 (over y, x), right: 8 (over z, core).
Axes of the slice: x: 4, y: 4, z: 4, core: 2. Of those that a mesh axis runs over, the one named last changes fastest.
Arguments:
- signal: float32 [512, 512, 2048], P(None, 'left', 'right'), may hold values from -6 to 6
- symbol_x: float32 [512], replicated, may hold values from 0.3 to 3
- symbol_y: float32 [512], replicated, may hold values from 0.3 to 3
- symbol_z: float32 [2048], replicated, may hold values from 0.3 to 3
Outputs:
- spectrum: float32 [256, 256, 1024], P('left', 'right')
The draws below stay inside these ranges and needn't reach their ends.
All inputs are finite; a program needn't handle non-finite values.
Results may differ from the reference program's by a relative error of at most 0.000096.
Values sent between devices are 32-bit elements; how exact they have to be, the bound alone decides.
A program may use at most 128 MiB of HBM per device.

```python
import jax
import jax.numpy as jnp
from jax import lax

GRID_X = 512
GRID_Y = 512
GRID_Z = 2048


def steps_of(stream_key, extent, shards, smallest, largest):
    gain = 1.0
    for position, blocks in shards:
        steps = jax.random.uniform(jax.random.fold_in(jax.random.fold_in(stream_key, 6), position), (blocks,), jnp.float32, smallest / len(shards), largest / len(shards))
        gain = gain * jnp.repeat(jnp.exp(steps), extent[position] // blocks).reshape((-1,) + (1,) * (len(extent) - 1 - position))
    return gain


def normal_values(stream_key, extent, spread, most, split=(), dtype=jnp.bfloat16):
    level = steps_of(stream_key, extent, split, -0.22, 0.18) if split else 1.0
    result = jax.random.normal(stream_key, extent, jnp.float32) * spread * level
    return jnp.minimum(jnp.maximum(result, -most), most).astype(dtype)


def setup_inputs(seed: int = 0) -> dict:
    splits = jax.random.split(jax.random.key(seed), 5)
    return {
        "signal": normal_values(splits[0], (GRID_X, GRID_Y, GRID_Z), 1.0, 6.0, ((1, 16), (2, 8)), jnp.float32),
        "symbol_x": jnp.clip(jax.random.uniform(splits[1], (GRID_X,), jnp.float32, 0.3, 3.0), 0.3, 3.0),
        "symbol_y": jnp.clip(jax.random.uniform(splits[2], (GRID_Y,), jnp.float32, 0.3, 3.0), 0.3, 3.0),
        "symbol_z": jnp.clip(jax.random.uniform(splits[3], (GRID_Z,), jnp.float32, 0.3, 3.0), 0.3, 3.0),
    }


def transform_table(count):
    rank = jnp.arange(count)
    angle = (jnp.pi / (4 * count)) * (((2 * rank[:, None] + 1) * (2 * rank[None, :] + 1)) % (8 * count)).astype(jnp.float32)
    return jnp.cos(angle) * (2.0 / count) ** 0.5


def transform_dim(values, dim):
    moved = jnp.tensordot(values, transform_table(values.shape[dim]), axes=([dim], [0]), precision=lax.Precision.HIGHEST)
    return jnp.moveaxis(moved, -1, dim)


def reference(signal, symbol_x, symbol_y, symbol_z):
    spectrum = signal
    spectrum = transform_dim(spectrum, 0)
    spectrum = lax.slice_in_dim(spectrum, 0, GRID_X // 2, axis=0)
    spectrum = transform_dim(spectrum, 1)
    spectrum = lax.slice_in_dim(spectrum, 0, GRID_Y // 2, axis=1)
    spectrum = transform_dim(spectrum, 2)
    spectrum = lax.slice_in_dim(spectrum, 0, GRID_Z // 2, axis=2)
    symbol = symbol_x[:GRID_X // 2][:, None, None] + symbol_y[:GRID_Y // 2][None, :, None] + symbol_z[:GRID_Z // 2][None, None, :]
    spectrum = spectrum * ((1.0 - 0.2 * symbol) / (1.0 + 0.2 * symbol))
    return spectrum
```

```python
import functools

import jax
import jax.numpy as jnp
import numpy as np
from jax import lax
from jax.experimental import pallas as pl
from jax.experimental.pallas import tpu as pltpu
from jax.sharding import PartitionSpec as P

MESH = pl.DeviceIdType.MESH
F32 = jnp.float32
BF16 = jnp.bfloat16
NX, NY, NZ = 512, 512, 2048
KX, KY, KZ = NX // 2, NY // 2, NZ // 2
LEFT, RIGHT = 16, 8
YL, ZL = NY // LEFT, NZ // RIGHT
XO, YO = KX // LEFT, KY // RIGHT
PITCH = 72
EARLY = 4
FINE = 64


def half_table(count):
    i = np.arange(count, dtype=np.int64)[:, None]
    k = np.arange(count // 2, dtype=np.int64)[None, :]
    phase = (2 * i + 1) * (2 * k + 1) % (8 * count)
    return np.cos(np.pi / (4 * count) * phase) * np.sqrt(2.0 / count)


def split_table(count):
    table = np.ascontiguousarray(half_table(count).T).astype(np.float32)
    high = table.astype(BF16)
    low = (table - high.astype(np.float32)).astype(BF16)
    return np.concatenate([high, high, low], axis=1)


def factor_tables(count):
    k = 2 * np.arange(count // 2, dtype=np.int64)[None, :] + 1
    a = np.arange(count // FINE, dtype=np.int64)[:, None]
    b = np.arange(FINE, dtype=np.int64)[:, None]
    coarse = np.pi / (4 * count) * (2 * FINE * a * k % (8 * count))
    fine = np.pi / (4 * count) * ((2 * b + 1) * k % (8 * count))
    scale = np.sqrt(2.0 / count)
    return (
        np.stack([np.cos(coarse) * scale, np.sin(coarse) * scale]).astype(np.float32),
        np.stack([np.cos(fine), np.sin(fine)]).astype(np.float32),
    )


def parts(values):
    high = values.astype(BF16)
    low = (values - high.astype(F32)).astype(BF16)
    return high, low


def dot(a, b):
    return jnp.dot(a, b, preferred_element_type=F32)


def kernel(
    s_ref, h_ref, coarse_ref, fine_ref, sx_ref, sy_ref, sz_ref, o_ref,
    slabs, table, coarse, fine, ztable, t1, r1, t2, q, zlhs, sym, result,
    slab_sem, table_sem, lsend, lrecv, qsend, qrecv, out_sem,
):
    left = lax.axis_index("left")
    right = lax.axis_index("right")
    cy, cx = left // 4, left % 4

    def left_peer(p, sign):
        return ((cy + sign * (p // 4) + 4) % 4) * 4 + (cx + sign * (p % 4) + 4) % 4

    def right_peer(p, sign):
        return ((right // 2 + sign * (p // 2) + 4) % 4) * 2 + (right + p) % 2

    barrier = pltpu.get_barrier_semaphore()
    for p in range(1, LEFT):
        pl.semaphore_signal(barrier, inc=1, device_id=(left_peer(p, -1), right), device_id_type=MESH)
    for p in range(1, RIGHT):
        pl.semaphore_signal(barrier, inc=1, device_id=(left, right_peer(p, -1)), device_id_type=MESH)

    def slab_copy(i):
        return pltpu.make_async_copy(
            s_ref.at[:, pl.ds(pl.multiple_of(i // 2 * 8, 8), 8), pl.ds(pl.multiple_of(i % 2 * 128, 128), 128)],
            slabs.at[i],
            slab_sem.at[i],
        )

    table_copies = [
        pltpu.make_async_copy(h_ref, table, table_sem.at[0]),
        pltpu.make_async_copy(coarse_ref, coarse, table_sem.at[1]),
        pltpu.make_async_copy(fine_ref, fine, table_sem.at[2]),
    ]
    table_copies[0].start()
    for i in range(8):
        slab_copy(i).start()
    table_copies[1].start()
    table_copies[2].start()
    table_copies[0].wait()

    def x_slab(i):
        slab_copy(i).wait()
        rows = slabs.at[i].reshape(NX * 8, 128)
        for pair in range(4):
            data = jnp.concatenate(
                [rows[pl.ds(2 * pair + e, NX, stride=8), :] for e in range(2)], axis=1
            )
            high, low = parts(data)
            modes = dot(table[...], jnp.concatenate([high, low, high], axis=0))
            for e in range(2):
                t1[pl.ds(i * 8 + 2 * pair + e, KX, stride=PITCH), :] = modes[:, 128 * e : 128 * (e + 1)]

    def left_copy(x, p, first, count):
        peer = left_peer(p, 1)
        return pltpu.make_async_remote_copy(
            src_ref=t1.at[pl.ds(pl.multiple_of((peer * XO + x) * PITCH + first, 8), count), :],
            dst_ref=r1.at[pl.ds(pl.multiple_of((x * LEFT + left) * 64 + first, 8), count), :],
            send_sem=lsend.at[x],
            recv_sem=lrecv.at[x],
            device_id=(peer, right),
            device_id_type=MESH,
        )

    def x_step(b, carry):
        x_slab(2 * b)
        x_slab(2 * b + 1)

        @pl.when(b == 0)
        def _():
            pl.semaphore_wait(barrier, LEFT + RIGHT - 2)

        def send(j, carry):
            left_copy(j // (LEFT - 1), j % (LEFT - 1) + 1, b * 16, 16).start()
            return carry

        lax.fori_loop(0, EARLY * (LEFT - 1), send, 0)
        return carry

    lax.fori_loop(0, 4, x_step, 0)

    def send(j, carry):
        left_copy(EARLY + j // (LEFT - 1), j % (LEFT - 1) + 1, 0, 64).start()
        return carry

    lax.fori_loop(0, (XO - EARLY) * (LEFT - 1), send, 0)

    def own(x, carry):
        r1[pl.ds(pl.multiple_of((x * LEFT + left) * 64, 8), 64), :] = t1[
            pl.ds(pl.multiple_of((left * XO + x) * PITCH, 8), 64), :
        ]
        return carry

    lax.fori_loop(0, XO, own, 0)

    table_copies[1].wait()
    table_copies[2].wait()

    def z_rows(a, carry):
        cos_a, sin_a = coarse[0, pl.ds(a, 1), :], coarse[1, pl.ds(a, 1), :]
        block = cos_a * fine[0] - sin_a * fine[1]
        high, low = parts(block)
        for n in range(4):
            ztable[n, pl.ds(pl.multiple_of(a * FINE, FINE), FINE), :] = high[:, 256 * n : 256 * (n + 1)]
            ztable[n, pl.ds(pl.multiple_of(NZ + a * FINE, FINE), FINE), :] = low[:, 256 * n : 256 * (n + 1)]
        return carry

    lax.fori_loop(0, NZ // FINE, z_rows, 0)

    row = lax.broadcasted_iota(jnp.int32, (YO, 128), 0)
    of_y = jnp.zeros((YO, 128), F32)
    for j in range(YO):
        of_y = jnp.where(row == j, sy_ref[right * YO + j], of_y)
    sym[...] = of_y

    def right_copy(x, p):
        peer = right_peer(p, 1)
        return pltpu.make_async_remote_copy(
            src_ref=t2.at[x, pl.ds(pl.multiple_of(peer * YO, YO), YO), :],
            dst_ref=q.at[x, right],
            send_sem=qsend.at[x],
            recv_sem=qrecv.at[x],
            device_id=(left, peer),
            device_id_type=MESH,
        )

    def out_copy(x):
        return pltpu.make_async_copy(result.at[x], o_ref.at[x], out_sem.at[x])

    def left_bytes(x):
        return r1.at[pl.ds(pl.multiple_of(x * 1024, 1024), 64 * (LEFT - 1)), :]

    def right_bytes(x):
        return q.at[x, pl.ds(0, RIGHT - 1)]

    def y_step(x):
        pltpu.make_async_copy(left_bytes(x), left_bytes(x), lrecv.at[x]).wait()
        lines = r1[pl.ds(pl.multiple_of(x * 1024, 1024), 1024), :].reshape(64, 2, 8, 128)
        data = jnp.concatenate([lines[:, e].reshape(NY, 128) for e in range(2)], axis=1)
        high, low = parts(data)
        t2[x] = dot(table[...], jnp.concatenate([high, low, high], axis=0))
        for p in range(1, RIGHT):
            right_copy(x, p).start()
        q[x, right] = t2[x, pl.ds(pl.multiple_of(right * YO, YO), YO), :]

    def z_step(x):
        pltpu.make_async_copy(right_bytes(x), right_bytes(x), qrecv.at[x]).wait()
        for k in range(RIGHT):
            high, low = parts(q[x, k])
            zlhs[0:YO, 256 * k : 256 * (k + 1)] = high
            zlhs[YO : 2 * YO, 256 * k : 256 * (k + 1)] = low
        of_xy = sx_ref[left * XO + x] + sym[...]
        of_xy = jnp.concatenate([of_xy, of_xy], axis=1)
        for n in range(4):
            both = dot(zlhs[...], ztable[n, 0:NZ, :])
            rest = dot(zlhs[0:YO, :], ztable[n, NZ : 2 * NZ, :])
            symbol = of_xy + sz_ref[:, 256 * n : 256 * (n + 1)]
            ratio = (1.0 - 0.2 * symbol) / (1.0 + 0.2 * symbol)
            result[x, :, 256 * n : 256 * (n + 1)] = (both[0:YO] + (both[YO:] + rest)) * ratio
        out_copy(x).start()

    def step(i, carry):
        @pl.when(i < XO)
        def _():
            y_step(i)

        @pl.when(i > 0)
        def _():
            z_step(i - 1)

        return carry

    lax.fori_loop(0, XO + 1, step, 0)

    def finish(x, carry):
        pltpu.make_async_copy(left_bytes(x), left_bytes(x), lsend.at[x]).wait()
        pltpu.make_async_copy(right_bytes(x), right_bytes(x), qsend.at[x]).wait()
        out_copy(x).wait()
        return carry

    lax.fori_loop(0, XO, finish, 0)


def body(signal, symbol_x, symbol_y, symbol_z):
    coarse, fine = factor_tables(NZ)
    table = split_table(NX)
    dma = pltpu.SemaphoreType.DMA
    any_space = pl.BlockSpec(memory_space=pl.ANY)
    smem = pl.BlockSpec(memory_space=pltpu.SMEM)
    return pl.pallas_call(
        kernel,
        out_shape=jax.ShapeDtypeStruct((XO, YO, KZ), F32),
        in_specs=[any_space, any_space, any_space, any_space, smem, smem, pl.BlockSpec(memory_space=pltpu.VMEM)],
        out_specs=any_space,
        scratch_shapes=[
            pltpu.VMEM((8, NX, 8, 128), F32),
            pltpu.VMEM(table.shape, BF16),
            pltpu.VMEM(coarse.shape, F32),
            pltpu.VMEM(fine.shape, F32),
            pltpu.VMEM((4, 2 * NZ, 256), BF16),
            pltpu.VMEM((KX * PITCH, 128), F32),
            pltpu.VMEM((XO * LEFT * 64, 128), F32),
            pltpu.VMEM((XO, KY, ZL), F32),
            pltpu.VMEM((XO, RIGHT, YO, ZL), F32),
            pltpu.VMEM((2 * YO, NZ), BF16),
            pltpu.VMEM((YO, 128), F32),
            pltpu.VMEM((XO, YO, KZ), F32),
            dma((8,)),
            dma((3,)),
            dma((XO,)),
            dma((XO,)),
            dma((XO,)),
            dma((XO,)),
            dma((XO,)),
        ],
        compiler_params=pltpu.CompilerParams(
            collective_id=0, has_side_effects=True, vmem_limit_bytes=67043328
        ),
    )(
        signal,
        jnp.asarray(table),
        jnp.asarray(coarse),
        jnp.asarray(fine),
        symbol_x,
        symbol_y,
        symbol_z.reshape(1, NZ),
    )


def solution(mesh):
    in_specs = (P(None, "left", "right"), P(), P(), P())
    out_specs = P("left", "right", None)
    return jax.shard_map(body, mesh=mesh, in_specs=in_specs, out_specs=out_specs, check_vma=False)
```

```python
import functools

import jax
import jax.numpy as jnp
import numpy as np
from jax import lax
from jax.experimental import pallas as pl
from jax.experimental.pallas import tpu as pltpu
from jax.sharding import PartitionSpec as P

MESH = pl.DeviceIdType.MESH
F32 = jnp.float32
BF16 = jnp.bfloat16
NX, NY, NZ = 512, 512, 2048
KX, KY, KZ = NX // 2, NY // 2, NZ // 2
LEFT, RIGHT = 16, 8
YL, ZL = NY // LEFT, NZ // RIGHT
XO, YO = KX // LEFT, KY // RIGHT
PITCH = 72
XA = XO - RIGHT
EARLY = 2
FINE = 64


def half_table(count):
    i = np.arange(count, dtype=np.int64)[:, None]
    k = np.arange(count // 2, dtype=np.int64)[None, :]
    phase = (2 * i + 1) * (2 * k + 1) % (8 * count)
    return np.cos(np.pi / (4 * count) * phase) * np.sqrt(2.0 / count)


def split_table(count, order):
    table = np.ascontiguousarray(half_table(count).T[order]).astype(np.float32)
    high = table.astype(BF16)
    low = (table - high.astype(np.float32)).astype(BF16)
    return np.concatenate([high, high, low], axis=1)


def x_order():
    block = np.arange(LEFT) * XO
    second = block[None, :] + XA + np.arange(RIGHT)[:, None]
    first = block[:, None] + np.arange(XA)[None, :]
    return np.concatenate([second.reshape(-1), first.reshape(-1)])


def factor_tables(count):
    k = 2 * np.arange(count // 2, dtype=np.int64)[None, :] + 1
    a = np.arange(count // FINE, dtype=np.int64)[:, None]
    b = np.arange(FINE, dtype=np.int64)[:, None]
    coarse = np.pi / (4 * count) * (2 * FINE * a * k % (8 * count))
    fine = np.pi / (4 * count) * ((2 * b + 1) * k % (8 * count))
    scale = np.sqrt(2.0 / count)
    return (
        np.stack([np.cos(coarse) * scale, np.sin(coarse) * scale]).astype(np.float32),
        np.stack([np.cos(fine), np.sin(fine)]).astype(np.float32),
    )


def parts(values):
    high = values.astype(BF16)
    low = (values - high.astype(F32)).astype(BF16)
    return high, low


def dot(a, b):
    return jnp.dot(a, b, preferred_element_type=F32)


def kernel(
    s_ref, hx_ref, hy_ref, coarse_ref, fine_ref, sx_ref, sy_ref, sz_ref, o_ref,
    slabs, xtable, ytable, coarse, fine, ztable, t1, r1, t2, q, w, v, u, t3, zlhs, sym, result,
    slab_sem, table_sem, lsend, lrecv, qsend, qrecv, wsend, wrecv, usend, urecv, bsend, brecv, out_sem,
):
    left = lax.axis_index("left")
    right = lax.axis_index("right")
    cy, cx = left // 4, left % 4

    def left_peer(p, sign):
        return ((cy + sign * (p // 4) + 4) % 4) * 4 + (cx + sign * (p % 4) + 4) % 4

    def right_peer(p, sign):
        return ((right // 2 + sign * (p // 2) + 4) % 4) * 2 + (right + p) % 2

    barrier = pltpu.get_barrier_semaphore()
    for p in range(1, LEFT):
        pl.semaphore_signal(barrier, inc=1, device_id=(left_peer(p, -1), right), device_id_type=MESH)
    for p in range(1, RIGHT):
        pl.semaphore_signal(barrier, inc=1, device_id=(left, right_peer(p, -1)), device_id_type=MESH)

    def slab_copy(i):
        return pltpu.make_async_copy(
            s_ref.at[:, pl.ds(pl.multiple_of(i // 2 * 8, 8), 8), pl.ds(pl.multiple_of(i % 2 * 128, 128), 128)],
            slabs.at[i],
            slab_sem.at[i],
        )

    table_copies = [
        pltpu.make_async_copy(hx_ref, xtable, table_sem.at[0]),
        pltpu.make_async_copy(coarse_ref, coarse, table_sem.at[1]),
        pltpu.make_async_copy(fine_ref, fine, table_sem.at[2]),
        pltpu.make_async_copy(hy_ref, ytable, table_sem.at[3]),
    ]
    slab_copy(0).start()
    table_copies[0].start()
    slab_copy(1).start()
    table_copies[0].wait()

    sym[...] = jnp.broadcast_to(sy_ref[:, 0:KY], (128, KY)).T

    def x_slab(i):
        rows = slabs.at[i].reshape(NX * 8, 128)
        lines = t1.reshape(KX * PITCH, 128)
        for pair in range(4):
            data = jnp.concatenate(
                [rows[pl.ds(2 * pair + e, NX, stride=8), :] for e in range(2)], axis=1
            )
            high, low = parts(data)
            modes = dot(xtable[...], jnp.concatenate([high, low, high], axis=0))
            for e in range(2):
                lines[pl.ds(i * 8 + 2 * pair + e, KX, stride=PITCH), :] = modes[:, 128 * e : 128 * (e + 1)]

    def left_copy(p, x, modes, first, count):
        peer = left_peer(p, 1)
        return pltpu.make_async_remote_copy(
            src_ref=t1.at[pl.ds(KX // 2 + peer * XA + x, modes), pl.ds(pl.multiple_of(first, 8), count), :],
            dst_ref=r1.at[pl.ds(x, modes), left, pl.ds(pl.multiple_of(first, 8), count), :],
            send_sem=lsend.at[x],
            recv_sem=lrecv.at[x],
            device_id=(peer, right),
            device_id_type=MESH,
        )

    def w_copy(b, half, d):
        peer = right_peer(d, 1)
        return pltpu.make_async_remote_copy(
            src_ref=t1.at[pl.ds(peer * LEFT + half * 8, 8), pl.ds(pl.multiple_of(b * 16, 16), 16), :],
            dst_ref=w.at[pl.ds((b * RIGHT + right) * LEFT + half * 8, 8)],
            send_sem=wsend.at[b],
            recv_sem=wrecv.at[b],
            device_id=(left, peer),
            device_id_type=MESH,
        )

    def x_step(b, carry):
        slab_copy(2 * b).wait()

        @pl.when(b < 3)
        def _():
            slab_copy(2 * b + 2).start()
            slab_copy(2 * b + 3).start()

        @pl.when(b == 3)
        def _():
            for copy in table_copies[1:]:
                copy.start()

        x_slab(2 * b)
        slab_copy(2 * b + 1).wait()
        x_slab(2 * b + 1)

        @pl.when(b == 0)
        def _():
            pl.semaphore_wait(barrier, LEFT + RIGHT - 2)

        def send_w(j, carry):
            w_copy(b, j // (RIGHT - 1), j % (RIGHT - 1) + 1).start()
            return carry

        def send_left(j, carry):
            left_copy(j + 1, 0, EARLY, b * 16, 16).start()
            return carry

        lax.fori_loop(0, 2 * (RIGHT - 1), send_w, 0)
        lax.fori_loop(0, LEFT - 1, send_left, 0)
        return carry

    lax.fori_loop(0, 4, x_step, 0)

    def send_left(j, carry):
        left_copy(j % (LEFT - 1) + 1, EARLY + j // (LEFT - 1), 1, 0, 64).start()
        return carry

    def own_left(x, carry):
        r1[x, left] = t1[KX // 2 + left * XA + x, 0:64, :]
        return carry

    lax.fori_loop(0, XA, own_left, 0)

    def own_w(j, carry):
        for b in range(4):
            w[(b * RIGHT + right) * LEFT + j] = t1[right * LEFT + j, 16 * b : 16 * (b + 1), :]
        return carry

    lax.fori_loop(0, LEFT, own_w, 0)

    table_copies[1].wait()
    table_copies[2].wait()
    table_copies[3].wait()

    def z_rows(a, carry):
        cos_a, sin_a = coarse[0, pl.ds(a, 1), :], coarse[1, pl.ds(a, 1), :]
        block = cos_a * fine[0] - sin_a * fine[1]
        high, low = parts(block)
        for n in range(4):
            ztable[n, pl.ds(pl.multiple_of(a * FINE, FINE), FINE), :] = high[:, 256 * n : 256 * (n + 1)]
            ztable[n, pl.ds(pl.multiple_of(NZ + a * FINE, FINE), FINE), :] = low[:, 256 * n : 256 * (n + 1)]
        return carry

    lax.fori_loop(0, NZ // FINE, z_rows, 0)

    def right_copy(x, d):
        peer = right_peer(d, 1)
        return pltpu.make_async_remote_copy(
            src_ref=t2.at[x, pl.ds(pl.multiple_of(peer * YO, YO), YO), :],
            dst_ref=q.at[x, right],
            send_sem=qsend.at[x],
            recv_sem=qrecv.at[x],
            device_id=(left, peer),
            device_id_type=MESH,
        )

    def u_copy(k, p):
        peer = left_peer(p, 1)
        return pltpu.make_async_remote_copy(
            src_ref=v.at[k, pl.ds(pl.multiple_of(peer * 8, 8), 8), :],
            dst_ref=u.at[pl.ds(pl.multiple_of(left * YL + 8 * k, 8), 8), :],
            send_sem=usend,
            recv_sem=urecv,
            device_id=(peer, right),
            device_id_type=MESH,
        )

    def b_copy(n, d):
        peer = right_peer(d, 1)
        return pltpu.make_async_remote_copy(
            src_ref=t3.at[pl.ds(pl.multiple_of(peer * YO, YO), YO), pl.ds(256 * n, 256)],
            dst_ref=result.at[XA + right, :, pl.ds(256 * n, 256)],
            send_sem=bsend,
            recv_sem=brecv,
            device_id=(left, peer),
            device_id_type=MESH,
        )

    def out_copy(k):
        return pltpu.make_async_copy(result.at[pl.ds(2 * k, 2)], o_ref.at[pl.ds(2 * k, 2)], out_sem.at[k])

    def arrived(ref, sem):
        pltpu.make_async_copy(ref, ref, sem).wait()

    def left_bytes(x, modes):
        return r1.at[pl.ds(x, modes), pl.ds(0, LEFT - 1)]

    def right_bytes(x):
        return q.at[x, pl.ds(0, RIGHT - 1)]

    def w_bytes(b):
        return w.at[pl.ds(b * RIGHT * LEFT, (RIGHT - 1) * LEFT)]

    def u_bytes():
        return u.at[pl.ds(0, NY - YL), :]

    def b_bytes():
        return result.at[pl.ds(XA, RIGHT - 1)]

    def ratio(of_xy, n):
        symbol = jnp.concatenate([of_xy, of_xy], axis=1) + sz_ref[:, 256 * n : 256 * (n + 1)]
        return (1.0 - 0.2 * symbol) / (1.0 + 0.2 * symbol)

    def z_modes(m, n):
        both = dot(zlhs[0 : 2 * m, :], ztable[n, 0:NZ, :])
        return both[0:m] + (both[m:] + dot(zlhs[0:m, :], ztable[n, NZ : 2 * NZ, :]))

    def y_of_first(x):
        @pl.when(x == 0)
        def _():
            arrived(left_bytes(0, EARLY), lrecv.at[0])

        @pl.when(x >= EARLY)
        def _():
            arrived(left_bytes(x, 1), lrecv.at[x])

        lines = r1[x].reshape(64, 2, 8, 128)
        data = jnp.concatenate([lines[:, e].reshape(NY, 128) for e in range(2)], axis=1)
        high, low = parts(data)
        t2[x] = dot(ytable[...], jnp.concatenate([high, low, high], axis=0))
        for d in range(1, RIGHT):
            right_copy(x, d).start()
        q[x, right] = t2[x, pl.ds(pl.multiple_of(right * YO, YO), YO), :]

    def z_of_first(k):
        for e in range(2):
            x = 2 * k + e
            arrived(right_bytes(x), qrecv.at[x])
            for j in range(RIGHT):
                high, low = parts(q[x, j])
                zlhs[32 * e : 32 * (e + 1), 256 * j : 256 * (j + 1)] = high
                zlhs[64 + 32 * e : 64 + 32 * (e + 1), 256 * j : 256 * (j + 1)] = low
        of_y = sym[pl.ds(pl.multiple_of(right * YO, YO), YO), :]
        for n in range(4):
            modes = z_modes(64, n)
            for e in range(2):
                x = 2 * k + e
                result[x, :, 256 * n : 256 * (n + 1)] = modes[32 * e : 32 * (e + 1)] * ratio(
                    sx_ref[left * XO + x] + of_y, n
                )
        out_copy(k).start()

    def z_of_second(k):
        arrived(w_bytes(k), wrecv.at[k])
        for j in range(RIGHT):
            lines = w[pl.ds((k * RIGHT + j) * LEFT, LEFT)].reshape(LEFT, 2, 8, 128)
            for half in range(2):
                high, low = parts(lines[:, half].reshape(128, 128))
                column = 256 * j + 128 * half
                zlhs[0:128, column : column + 128] = high
                zlhs[128:256, column : column + 128] = low
        for n in range(4):
            v[k, :, 256 * n : 256 * (n + 1)] = z_modes(128, n)

        def send(p, carry):
            u_copy(k, p).start()
            return carry

        lax.fori_loop(1, LEFT, send, 0)
        u[pl.ds(pl.multiple_of(left * YL + 8 * k, 8), 8), :] = v[k, pl.ds(pl.multiple_of(left * 8, 8), 8), :]

    def y_of_second():
        arrived(u_bytes(), urecv)
        of_xy = sx_ref[left * XO + XA + right] + sym[...]
        for n in range(4):
            high, low = parts(u[:, 256 * n : 256 * (n + 1)])
            modes = dot(ytable[...], jnp.concatenate([high, low, high], axis=0))
            t3[:, 256 * n : 256 * (n + 1)] = modes * ratio(of_xy, n)
            for d in range(1, RIGHT):
                b_copy(n, d).start()
        result[XA + right] = t3[pl.ds(pl.multiple_of(right * YO, YO), YO), :]

    def step(i, carry):
        @pl.when(i < 4)
        def _():
            z_of_second(i)
            sends = jnp.where(i < 3, i + 1, XA - EARLY) * (LEFT - 1)
            lax.fori_loop(i * (LEFT - 1), sends, send_left, 0)

        @pl.when(i == 4)
        def _():
            y_of_second()

        @pl.when(i == 7)
        def _():
            arrived(b_bytes(), brecv)
            for k in range(XA // 2, XO // 2):
                out_copy(k).start()

        def first(x, carry):
            y_of_first(x)
            return carry

        lax.fori_loop(jnp.where(i == 0, 0, i + 1), jnp.minimum(i + 2, XA), first, 0)

        @pl.when(i >= 4)
        def _():
            z_of_first(i - 4)

        return carry

    lax.fori_loop(0, 8, step, 0)

    def sent_first(x, carry):
        @pl.when(x == 0)
        def _():
            arrived(left_bytes(0, EARLY), lsend.at[0])

        @pl.when(x >= EARLY)
        def _():
            arrived(left_bytes(x, 1), lsend.at[x])

        arrived(right_bytes(x), qsend.at[x])
        return carry

    def sent_second(p, carry):
        arrived(w_bytes(p), wsend.at[p])
        return carry

    lax.fori_loop(0, XA, sent_first, 0)
    lax.fori_loop(0, 4, sent_second, 0)
    arrived(u_bytes(), usend)
    arrived(b_bytes(), bsend)
    for k in range(XO // 2):
        out_copy(k).wait()


def body(signal, symbol_x, symbol_y, symbol_z):
    coarse, fine = factor_tables(NZ)
    xtable = split_table(NX, x_order())
    ytable = split_table(NY, np.arange(KY))
    dma = pltpu.SemaphoreType.DMA
    any_space = pl.BlockSpec(memory_space=pl.ANY)
    smem = pl.BlockSpec(memory_space=pltpu.SMEM)
    vmem = pl.BlockSpec(memory_space=pltpu.VMEM)
    return pl.pallas_call(
        kernel,
        out_shape=jax.ShapeDtypeStruct((XO, YO, KZ), F32),
        in_specs=[any_space, any_space, any_space, any_space, any_space, smem, vmem, vmem],
        out_specs=any_space,
        scratch_shapes=[
            pltpu.VMEM((8, NX, 8, 128), F32),
            pltpu.VMEM(xtable.shape, BF16),
            pltpu.VMEM(ytable.shape, BF16),
            pltpu.VMEM(coarse.shape, F32),
            pltpu.VMEM(fine.shape, F32),
            pltpu.VMEM((4, 2 * NZ, 256), BF16),
            pltpu.VMEM((KX, PITCH, 128), F32),
            pltpu.VMEM((XA, LEFT, 64, 128), F32),
            pltpu.VMEM((XA, KY, ZL), F32),
            pltpu.VMEM((XA, RIGHT, YO, ZL), F32),
            pltpu.VMEM((4 * RIGHT * LEFT, 16, 128), F32),
            pltpu.VMEM((4, 8 * LEFT, KZ), F32),
            pltpu.VMEM((NY, KZ), F32),
            pltpu.VMEM((KY, KZ), F32),
            pltpu.VMEM((256, NZ), BF16),
            pltpu.VMEM((KY, 128), F32),
            pltpu.VMEM((XO, YO, KZ), F32),
            dma((8,)),
            dma((4,)),
            dma((XA,)),
            dma((XA,)),
            dma((XA,)),
            dma((XA,)),
            dma((4,)),
            dma((4,)),
            dma(()),
            dma(()),
            dma(()),
            dma(()),
            dma((XO // 2,)),
        ],
        compiler_params=pltpu.CompilerParams(
            collective_id=0, has_side_effects=True, vmem_limit_bytes=67043328
        ),
    )(
        signal,
        jnp.asarray(xtable),
        jnp.asarray(ytable),
        jnp.asarray(coarse),
        jnp.asarray(fine),
        symbol_x,
        symbol_y.reshape(1, NY),
        symbol_z.reshape(1, NZ),
    )


def solution(mesh):
    in_specs = (P(None, "left", "right"), P(), P(), P())
    out_specs = P("left", "right", None)
    return jax.shard_map(body, mesh=mesh, in_specs=in_specs, out_specs=out_specs, check_vma=False)
```

```python
import functools

import jax
import jax.numpy as jnp
import numpy as np
from jax import lax
from jax.experimental import pallas as pl
from jax.experimental.pallas import tpu as pltpu
from jax.sharding import PartitionSpec as P

MESH = pl.DeviceIdType.MESH
F32 = jnp.float32
BF16 = jnp.bfloat16
NX, NY, NZ = 512, 512, 2048
KX, KY, KZ = NX // 2, NY // 2, NZ // 2
LEFT, RIGHT = 16, 8
YL, ZL = NY // LEFT, NZ // RIGHT
XO, YO = KX // LEFT, KY // RIGHT
PITCH = 72
XA = XO - RIGHT
EARLY = 2
FINE = 64


def half_table(count):
    i = np.arange(count, dtype=np.int64)[:, None]
    k = np.arange(count // 2, dtype=np.int64)[None, :]
    phase = (2 * i + 1) * (2 * k + 1) % (8 * count)
    return np.cos(np.pi / (4 * count) * phase) * np.sqrt(2.0 / count)


def split_table(count, order):
    table = np.ascontiguousarray(half_table(count).T[order]).astype(np.float32)
    high = table.astype(BF16)
    low = (table - high.astype(np.float32)).astype(BF16)
    return np.concatenate([high, high, low], axis=1)


def x_order():
    block = np.arange(LEFT) * XO
    second = block[None, :] + XA + np.arange(RIGHT)[:, None]
    first = block[:, None] + np.arange(XA)[None, :]
    return np.concatenate([second.reshape(-1), first.reshape(-1)])


def factor_tables(count):
    k = 2 * np.arange(count // 2, dtype=np.int64)[None, :] + 1
    a = np.arange(count // FINE, dtype=np.int64)[:, None]
    b = np.arange(FINE, dtype=np.int64)[:, None]
    coarse = np.pi / (4 * count) * (2 * FINE * a * k % (8 * count))
    fine = np.pi / (4 * count) * ((2 * b + 1) * k % (8 * count))
    scale = np.sqrt(2.0 / count)
    return (
        np.stack([np.cos(coarse) * scale, np.sin(coarse) * scale]).astype(np.float32),
        np.stack([np.cos(fine), np.sin(fine)]).astype(np.float32),
    )


def parts(values):
    high = values.astype(BF16)
    low = (values - high.astype(F32)).astype(BF16)
    return high, low


def dot(a, b):
    return jnp.dot(a, b, preferred_element_type=F32)


def kernel(
    s_ref, hx_ref, hy_ref, coarse_ref, fine_ref, x_ref, y_ref, z_ref, result,
    slabs, xtable, ytable, coarse, fine, ztable, t1, r1, t2, q, w, v, u, t3, zlhs, sym, sx, sy, sz,
    slab_sem, table_sem, lsend, lrecv, qsend, qrecv, wsend, wrecv, usend, urecv, bsend, brecv,
):
    left = lax.axis_index("left")
    right = lax.axis_index("right")
    cy, cx = left // 4, left % 4

    def left_peer(p, sign):
        return ((cy + sign * (p // 4) + 4) % 4) * 4 + (cx + sign * (p % 4) + 4) % 4

    def right_peer(p, sign):
        return ((right // 2 + sign * (p // 2) + 4) % 4) * 2 + (right + p) % 2

    barrier = pltpu.get_barrier_semaphore()
    for p in range(1, LEFT):
        pl.semaphore_signal(barrier, inc=1, device_id=(left_peer(p, -1), right), device_id_type=MESH)
    for p in range(1, RIGHT):
        pl.semaphore_signal(barrier, inc=1, device_id=(left, right_peer(p, -1)), device_id_type=MESH)

    def slab_copy(i):
        return pltpu.make_async_copy(
            s_ref.at[:, pl.ds(pl.multiple_of(i // 2 * 8, 8), 8), pl.ds(pl.multiple_of(i % 2 * 128, 128), 128)],
            slabs.at[i],
            slab_sem.at[i],
        )

    table_copies = [
        pltpu.make_async_copy(hx_ref, xtable, table_sem.at[0]),
        pltpu.make_async_copy(coarse_ref, coarse, table_sem.at[1]),
        pltpu.make_async_copy(fine_ref, fine, table_sem.at[2]),
        pltpu.make_async_copy(hy_ref, ytable, table_sem.at[3]),
        pltpu.make_async_copy(x_ref, sx, table_sem.at[4]),
        pltpu.make_async_copy(y_ref, sy, table_sem.at[5]),
        pltpu.make_async_copy(z_ref, sz, table_sem.at[6]),
    ]
    slab_copy(0).start()
    table_copies[0].start()
    slab_copy(1).start()
    table_copies[0].wait()

    def x_slab(i):
        rows = slabs.at[i].reshape(NX * 8, 128)
        lines = t1.reshape(KX * PITCH, 128)
        for pair in range(4):
            data = jnp.concatenate(
                [rows[pl.ds(2 * pair + e, NX, stride=8), :] for e in range(2)], axis=1
            )
            high, low = parts(data)
            modes = dot(xtable[...], jnp.concatenate([high, low, high], axis=0))
            for e in range(2):
                lines[pl.ds(i * 8 + 2 * pair + e, KX, stride=PITCH), :] = modes[:, 128 * e : 128 * (e + 1)]

    def left_copy(p, x, modes, first, count):
        peer = left_peer(p, 1)
        return pltpu.make_async_remote_copy(
            src_ref=t1.at[pl.ds(KX // 2 + peer * XA + x, modes), pl.ds(pl.multiple_of(first, 8), count), :],
            dst_ref=r1.at[pl.ds(x, modes), left, pl.ds(pl.multiple_of(first, 8), count), :],
            send_sem=lsend.at[x],
            recv_sem=lrecv.at[x],
            device_id=(peer, right),
            device_id_type=MESH,
        )

    def w_copy(i, d):
        peer = right_peer(d, 1)
        return pltpu.make_async_remote_copy(
            src_ref=t1.at[pl.ds(peer * LEFT, LEFT), pl.ds(pl.multiple_of(i * 8, 8), 8), :],
            dst_ref=w.at[pl.ds((i // 2 * RIGHT + right) * LEFT, LEFT), pl.ds(pl.multiple_of(i % 2 * 8, 8), 8), :],
            send_sem=wsend.at[i // 2],
            recv_sem=wrecv.at[i // 2],
            device_id=(left, peer),
            device_id_type=MESH,
        )

    def x_step(b, carry):
        slab_copy(2 * b).wait()

        @pl.when(b < 3)
        def _():
            slab_copy(2 * b + 2).start()
            slab_copy(2 * b + 3).start()

        @pl.when(b == 3)
        def _():
            for copy in table_copies[1:]:
                copy.start()

        x_slab(2 * b)

        @pl.when(b == 0)
        def _():
            pl.semaphore_wait(barrier, LEFT + RIGHT - 2)

        for d in range(1, RIGHT):
            w_copy(2 * b, d).start()
        slab_copy(2 * b + 1).wait()
        x_slab(2 * b + 1)
        for d in range(1, RIGHT):
            w_copy(2 * b + 1, d).start()

        def send_left(j, carry):
            left_copy(j + 1, 0, EARLY, b * 16, 16).start()
            return carry

        lax.fori_loop(0, LEFT - 1, send_left, 0)
        return carry

    lax.fori_loop(0, 4, x_step, 0)

    def send_left(j, carry):
        left_copy(j % (LEFT - 1) + 1, EARLY + j // (LEFT - 1), 1, 0, 64).start()
        return carry

    lax.fori_loop(0, LEFT - 1, send_left, 0)

    def own_left(x, carry):
        r1[x, left] = t1[KX // 2 + left * XA + x, 0:64, :]
        return carry

    lax.fori_loop(0, XA, own_left, 0)

    def own_w(j, carry):
        for b in range(4):
            w[(b * RIGHT + right) * LEFT + j] = t1[right * LEFT + j, 16 * b : 16 * (b + 1), :]
        return carry

    lax.fori_loop(0, LEFT, own_w, 0)

    for copy in table_copies[1:]:
        copy.wait()
    sym[...] = jnp.broadcast_to(sy[:, 0:KY], (128, KY)).T

    def z_rows(a, carry):
        cos_a, sin_a = coarse[0, pl.ds(a, 1), :], coarse[1, pl.ds(a, 1), :]
        block = cos_a * fine[0] - sin_a * fine[1]
        high, low = parts(block)
        for n in range(4):
            ztable[n, pl.ds(pl.multiple_of(a * FINE, FINE), FINE), :] = high[:, 256 * n : 256 * (n + 1)]
            ztable[n, pl.ds(pl.multiple_of(NZ + a * FINE, FINE), FINE), :] = low[:, 256 * n : 256 * (n + 1)]
        return carry

    lax.fori_loop(0, NZ // FINE, z_rows, 0)

    def right_copy(x, d):
        peer = right_peer(d, 1)
        return pltpu.make_async_remote_copy(
            src_ref=t2.at[x, pl.ds(pl.multiple_of(peer * YO, YO), YO), :],
            dst_ref=q.at[x, right],
            send_sem=qsend.at[x],
            recv_sem=qrecv.at[x],
            device_id=(left, peer),
            device_id_type=MESH,
        )

    def u_copy(k, p):
        peer = left_peer(p, 1)
        return pltpu.make_async_remote_copy(
            src_ref=v.at[k, pl.ds(pl.multiple_of(peer * 8, 8), 8), :],
            dst_ref=u.at[pl.ds(pl.multiple_of(left * YL + 8 * k, 8), 8), :],
            send_sem=usend,
            recv_sem=urecv,
            device_id=(peer, right),
            device_id_type=MESH,
        )

    def b_copy(n, d):
        peer = right_peer(d, 1)
        return pltpu.make_async_remote_copy(
            src_ref=t3.at[pl.ds(pl.multiple_of(peer * YO, YO), YO), pl.ds(pl.multiple_of(256 * n, 256), 256)],
            dst_ref=result.at[XA + right, :, pl.ds(pl.multiple_of(256 * n, 256), 256)],
            send_sem=bsend,
            recv_sem=brecv,
            device_id=(left, peer),
            device_id_type=MESH,
        )

    def arrived(ref, sem):
        pltpu.make_async_copy(ref, ref, sem).wait()

    def left_bytes(x, modes):
        return r1.at[pl.ds(x, modes), pl.ds(0, LEFT - 1)]

    def right_bytes(x):
        return q.at[x, pl.ds(0, RIGHT - 1)]

    def w_bytes(b):
        return w.at[pl.ds(b * RIGHT * LEFT, (RIGHT - 1) * LEFT)]

    def u_bytes():
        return u.at[pl.ds(0, NY - YL), :]

    def b_bytes():
        return result.at[pl.ds(XA, RIGHT - 1)]

    def ratio(of_xy, n):
        symbol = jnp.concatenate([of_xy, of_xy], axis=1) + sz[:, 256 * n : 256 * (n + 1)]
        return (1.0 - 0.2 * symbol) / (1.0 + 0.2 * symbol)

    def z_modes(m, n):
        both = dot(zlhs[0 : 2 * m, :], ztable[n, 0:NZ, :])
        return both[0:m] + (both[m:] + dot(zlhs[0:m, :], ztable[n, NZ : 2 * NZ, :]))

    def y_of_first(x):
        @pl.when(x == 0)
        def _():
            arrived(left_bytes(0, EARLY), lrecv.at[0])

        @pl.when(x >= EARLY)
        def _():
            arrived(left_bytes(x, 1), lrecv.at[x])

        lines = r1[x].reshape(64, 2, 8, 128)
        data = jnp.concatenate([lines[:, e].reshape(NY, 128) for e in range(2)], axis=1)
        high, low = parts(data)
        t2[x] = dot(ytable[...], jnp.concatenate([high, low, high], axis=0))
        for d in range(1, RIGHT):
            right_copy(x, d).start()
        q[x, right] = t2[x, pl.ds(pl.multiple_of(right * YO, YO), YO), :]

    def z_of_first(k):
        for e in range(2):
            x = 2 * k + e
            arrived(right_bytes(x), qrecv.at[x])
            for j in range(RIGHT):
                high, low = parts(q[x, j])
                zlhs[32 * e : 32 * (e + 1), 256 * j : 256 * (j + 1)] = high
                zlhs[64 + 32 * e : 64 + 32 * (e + 1), 256 * j : 256 * (j + 1)] = low
        of_y = sym[pl.ds(pl.multiple_of(right * YO, YO), YO), :]
        for n in range(4):
            modes = z_modes(64, n)
            for e in range(2):
                x = 2 * k + e
                result[x, :, 256 * n : 256 * (n + 1)] = modes[32 * e : 32 * (e + 1)] * ratio(
                    sx[left * XO + x] + of_y, n
                )

    def z_of_second(k):
        arrived(w_bytes(k), wrecv.at[k])
        for j in range(RIGHT):
            lines = w[pl.ds((k * RIGHT + j) * LEFT, LEFT)].reshape(LEFT, 2, 8, 128)
            for half in range(2):
                high, low = parts(lines[:, half].reshape(128, 128))
                column = 256 * j + 128 * half
                zlhs[0:128, column : column + 128] = high
                zlhs[128:256, column : column + 128] = low
        for n in range(4):
            v[k, :, 256 * n : 256 * (n + 1)] = z_modes(128, n)

        def send(p, carry):
            u_copy(k, p).start()
            return carry

        lax.fori_loop(1, LEFT, send, 0)
        u[pl.ds(pl.multiple_of(left * YL + 8 * k, 8), 8), :] = v[k, pl.ds(pl.multiple_of(left * 8, 8), 8), :]

    def y_of_second():
        arrived(u_bytes(), urecv)
        of_xy = sx[left * XO + XA + right] + sym[...]
        for n in range(4):
            high, low = parts(u[:, 256 * n : 256 * (n + 1)])
            modes = dot(ytable[...], jnp.concatenate([high, low, high], axis=0))
            t3[:, 256 * n : 256 * (n + 1)] = modes * ratio(of_xy, n)
            if n < 2:
                for d in range(1, RIGHT):
                    b_copy(n, d).start()
        result[XA + right] = t3[pl.ds(pl.multiple_of(right * YO, YO), YO), :]

    def step(i, carry):
        @pl.when(i < 4)
        def _():
            z_of_second(i)
            first = i + 1
            last = jnp.where(i < 3, i + 2, XA - EARLY)
            lax.fori_loop(first * (LEFT - 1), last * (LEFT - 1), send_left, 0)

        @pl.when(i == 4)
        def _():
            y_of_second()

        @pl.when(i >= 4)
        def _():
            z_of_first(i - 4)

        def first(x, carry):
            y_of_first(x)
            return carry

        lax.fori_loop(jnp.where(i < 2, 2 * i, jnp.minimum(i + 2, XA)), jnp.where(i < 1, 2, jnp.minimum(i + 3, XA)), first, 0)

        @pl.when((i == 4) | (i == 5))
        def _():
            for d in range(1, RIGHT):
                b_copy(i - 2, d).start()

        return carry

    lax.fori_loop(0, 8, step, 0)
    arrived(b_bytes(), brecv)

    def sent_first(x, carry):
        @pl.when(x == 0)
        def _():
            arrived(left_bytes(0, EARLY), lsend.at[0])

        @pl.when(x >= EARLY)
        def _():
            arrived(left_bytes(x, 1), lsend.at[x])

        arrived(right_bytes(x), qsend.at[x])
        return carry

    def sent_second(p, carry):
        arrived(w_bytes(p), wsend.at[p])
        return carry

    lax.fori_loop(0, XA, sent_first, 0)
    lax.fori_loop(0, 4, sent_second, 0)
    arrived(u_bytes(), usend)
    arrived(b_bytes(), bsend)


def body(signal, symbol_x, symbol_y, symbol_z):
    coarse, fine = factor_tables(NZ)
    xtable = split_table(NX, x_order())
    ytable = split_table(NY, np.arange(KY))
    dma = pltpu.SemaphoreType.DMA
    any_space = pl.BlockSpec(memory_space=pl.ANY)
    vmem = pl.BlockSpec(memory_space=pltpu.VMEM)
    return pl.pallas_call(
        kernel,
        out_shape=pltpu.VMEM((XO, YO, KZ), F32),
        in_specs=[any_space] * 8,
        out_specs=vmem,
        scratch_shapes=[
            pltpu.VMEM((8, NX, 8, 128), F32),
            pltpu.VMEM(xtable.shape, BF16),
            pltpu.VMEM(ytable.shape, BF16),
            pltpu.VMEM(coarse.shape, F32),
            pltpu.VMEM(fine.shape, F32),
            pltpu.VMEM((4, 2 * NZ, 256), BF16),
            pltpu.VMEM((KX, PITCH, 128), F32),
            pltpu.VMEM((XA, LEFT, 64, 128), F32),
            pltpu.VMEM((XA, KY, ZL), F32),
            pltpu.VMEM((XA, RIGHT, YO, ZL), F32),
            pltpu.VMEM((4 * RIGHT * LEFT, 16, 128), F32),
            pltpu.VMEM((4, 8 * LEFT, KZ), F32),
            pltpu.VMEM((NY, KZ), F32),
            pltpu.VMEM((KY, KZ), F32),
            pltpu.VMEM((256, NZ), BF16),
            pltpu.VMEM((KY, 128), F32),
            pltpu.SMEM((NX,), F32),
            pltpu.VMEM((1, NY), F32),
            pltpu.VMEM((1, NZ), F32),
            dma((8,)),
            dma((7,)),
            dma((XA,)),
            dma((XA,)),
            dma((XA,)),
            dma((XA,)),
            dma((4,)),
            dma((4,)),
            dma(()),
            dma(()),
            dma(()),
            dma(()),
        ],
        compiler_params=pltpu.CompilerParams(
            collective_id=0, has_side_effects=True, vmem_limit_bytes=58 * 2**20
        ),
    )(
        signal,
        jnp.asarray(xtable),
        jnp.asarray(ytable),
        jnp.asarray(coarse),
        jnp.asarray(fine),
        symbol_x,
        symbol_y.reshape(1, NY),
        symbol_z.reshape(1, NZ),
    )


def solution(mesh):
    in_specs = (P(None, "left", "right"), P(), P(), P())
    out_specs = P("left", "right", None)
    return jax.shard_map(body, mesh=mesh, in_specs=in_specs, out_specs=out_specs, check_vma=False)
```

```python
import functools

import jax
import jax.numpy as jnp
import numpy as np
from jax import lax
from jax.experimental import pallas as pl
from jax.experimental.pallas import tpu as pltpu
from jax.sharding import PartitionSpec as P

MESH = pl.DeviceIdType.MESH
F32 = jnp.float32
BF16 = jnp.bfloat16
NX, NY, NZ = 512, 512, 2048
KX, KY, KZ = NX // 2, NY // 2, NZ // 2
LEFT, RIGHT = 16, 8
YL, ZL = NY // LEFT, NZ // RIGHT
XO, YO = KX // LEFT, KY // RIGHT
PITCH = 72
XA = XO - RIGHT
EARLY = 2
FINE = 64


def half_table(count):
    i = np.arange(count, dtype=np.int64)[:, None]
    k = np.arange(count // 2, dtype=np.int64)[None, :]
    phase = (2 * i + 1) * (2 * k + 1) % (8 * count)
    return np.cos(np.pi / (4 * count) * phase) * np.sqrt(2.0 / count)


def split_table(count, order):
    table = np.ascontiguousarray(half_table(count).T[order]).astype(np.float32)
    high = table.astype(BF16)
    low = (table - high.astype(np.float32)).astype(BF16)
    return np.concatenate([high, high, low], axis=1)


def x_order():
    block = np.arange(LEFT) * XO
    second = block[None, :] + XA + np.arange(RIGHT)[:, None]
    first = block[:, None] + np.arange(XA)[None, :]
    return np.concatenate([second.reshape(-1), first.reshape(-1)])


def factor_tables(count):
    k = 2 * np.arange(count // 2, dtype=np.int64)[None, :] + 1
    a = np.arange(count // FINE, dtype=np.int64)[:, None]
    b = np.arange(FINE, dtype=np.int64)[:, None]
    coarse = np.pi / (4 * count) * (2 * FINE * a * k % (8 * count))
    fine = np.pi / (4 * count) * ((2 * b + 1) * k % (8 * count))
    scale = np.sqrt(2.0 / count)
    return (
        np.stack([np.cos(coarse) * scale, np.sin(coarse) * scale]).astype(np.float32),
        np.stack([np.cos(fine), np.sin(fine)]).astype(np.float32),
    )


def parts(values):
    high = values.astype(BF16)
    low = (values - high.astype(F32)).astype(BF16)
    return high, low


def dot(a, b):
    return jnp.dot(a, b, preferred_element_type=F32)


def kernel(
    s_ref, hx_ref, hy_ref, coarse_ref, fine_ref, x_ref, y_ref, z_ref, result,
    slabs, xtable, ytable, coarse, fine, ztable, t1, r1, t2, q, w, v, u, t3, zlhs, sym, sx, sy, sz,
    ready, slab_sem, table_sem, lsend, lrecv, qsend, qrecv, wsend, wrecv, usend, urecv, bsend, brecv,
):
    left = lax.axis_index("left")
    right = lax.axis_index("right")
    cy, cx = left // 4, left % 4

    def left_peer(p, sign):
        return ((cy + sign * (p // 4) + 4) % 4) * 4 + (cx + sign * (p % 4) + 4) % 4

    def right_peer(p, sign):
        return ((right // 2 + sign * (p // 2) + 4) % 4) * 2 + (right + p) % 2

    def plane_peer(d, along):
        return left_peer(4 * d if along == 0 else d, 1)

    barrier = pltpu.get_barrier_semaphore()
    for d in range(1, RIGHT):
        pl.semaphore_signal(barrier, inc=1, device_id=(left, right_peer(d, -1)), device_id_type=MESH)
    for along in range(2):
        for d in range(1, 4):
            pl.semaphore_signal(barrier, inc=1, device_id=(plane_peer(d, along), right), device_id_type=MESH)

    def slab_copy(i):
        return pltpu.make_async_copy(
            s_ref.at[:, pl.ds(pl.multiple_of(i // 2 * 8, 8), 8), pl.ds(pl.multiple_of(i % 2 * 128, 128), 128)],
            slabs.at[i],
            slab_sem.at[i],
        )

    table_copies = [
        pltpu.make_async_copy(hx_ref, xtable, table_sem.at[0]),
        pltpu.make_async_copy(coarse_ref, coarse, table_sem.at[1]),
        pltpu.make_async_copy(fine_ref, fine, table_sem.at[2]),
        pltpu.make_async_copy(hy_ref, ytable, table_sem.at[3]),
        pltpu.make_async_copy(x_ref, sx, table_sem.at[4]),
        pltpu.make_async_copy(y_ref, sy, table_sem.at[5]),
        pltpu.make_async_copy(z_ref, sz, table_sem.at[6]),
    ]
    slab_copy(0).start()
    table_copies[0].start()
    slab_copy(1).start()
    table_copies[0].wait()

    def x_slab(i, first, last):
        rows = slabs.at[i].reshape(NX * 8, 128)
        lines = t1.reshape(KX * PITCH, 128)
        for pair in range(4):
            data = jnp.concatenate(
                [rows[pl.ds(2 * pair + e, NX, stride=8), :] for e in range(2)], axis=1
            )
            high, low = parts(data)
            modes = dot(xtable[first:last, :], jnp.concatenate([high, low, high], axis=0))
            for e in range(2):
                start = first * PITCH + i * 8 + 2 * pair + e
                lines[pl.ds(start, last - first, stride=PITCH), :] = modes[:, 128 * e : 128 * (e + 1)]

    def left_copy(p, x, modes, first, count):
        peer = left_peer(p, 1)
        return pltpu.make_async_remote_copy(
            src_ref=t1.at[pl.ds(KX // 2 + peer * XA + x, modes), pl.ds(pl.multiple_of(first, 8), count), :],
            dst_ref=r1.at[pl.ds(x, modes), left, pl.ds(pl.multiple_of(first, 8), count), :],
            send_sem=lsend.at[x],
            recv_sem=lrecv.at[x],
            device_id=(peer, right),
            device_id_type=MESH,
        )

    def w_copy(i, d):
        peer = right_peer(d, 1)
        return pltpu.make_async_remote_copy(
            src_ref=t1.at[pl.ds(peer * LEFT, LEFT), pl.ds(pl.multiple_of(i * 8, 8), 8), :],
            dst_ref=w.at[pl.ds((i // 2 * RIGHT + right) * LEFT, LEFT), pl.ds(pl.multiple_of(i % 2 * 8, 8), 8), :],
            send_sem=wsend.at[i // 2],
            recv_sem=wrecv.at[i // 2],
            device_id=(left, peer),
            device_id_type=MESH,
        )

    def send_w(i):
        for d in range(1, RIGHT):
            w_copy(i, d).start()

    def send_early(b):
        def send(j, carry):
            left_copy(j + 1, 0, EARLY, b * 16, 16).start()
            return carry

        lax.fori_loop(0, LEFT - 1, send, 0)

    slab_copy(0).wait()
    slab_copy(2).start()
    slab_copy(3).start()
    x_slab(0, 0, KX // 2)
    pl.semaphore_wait(barrier, RIGHT - 1 + 6)
    for d in range(1, 4):
        pl.semaphore_signal(ready, inc=1, device_id=(plane_peer(d, 1), right), device_id_type=MESH)
    send_w(0)
    x_slab(0, KX // 2, KX)
    slab_copy(1).wait()
    x_slab(1, 0, KX)
    send_w(1)
    pl.semaphore_wait(ready, 3)
    send_early(0)

    def x_step(b, carry):
        slab_copy(2 * b).wait()

        @pl.when(b < 3)
        def _():
            slab_copy(2 * b + 2).start()
            slab_copy(2 * b + 3).start()

        @pl.when(b == 3)
        def _():
            for copy in table_copies[1:]:
                copy.start()

        x_slab(2 * b, 0, KX)
        send_w(2 * b)
        slab_copy(2 * b + 1).wait()
        x_slab(2 * b + 1, 0, KX)
        send_w(2 * b + 1)
        send_early(b)
        return carry

    lax.fori_loop(1, 4, x_step, 0)

    def send_left(j, carry):
        left_copy(j % (LEFT - 1) + 1, EARLY + j // (LEFT - 1), 1, 0, 64).start()
        return carry

    lax.fori_loop(0, LEFT - 1, send_left, 0)

    def own_left(x, carry):
        r1[x, left] = t1[KX // 2 + left * XA + x, 0:64, :]
        return carry

    lax.fori_loop(0, XA, own_left, 0)

    def own_w(j, carry):
        for b in range(4):
            w[(b * RIGHT + right) * LEFT + j] = t1[right * LEFT + j, 16 * b : 16 * (b + 1), :]
        return carry

    lax.fori_loop(0, LEFT, own_w, 0)

    for copy in table_copies[1:]:
        copy.wait()
    sym[...] = jnp.broadcast_to(sy[:, 0:KY], (128, KY)).T

    def z_rows(a, carry):
        cos_a, sin_a = coarse[0, pl.ds(a, 1), :], coarse[1, pl.ds(a, 1), :]
        block = cos_a * fine[0] - sin_a * fine[1]
        high, low = parts(block)
        for n in range(4):
            ztable[n, pl.ds(pl.multiple_of(a * FINE, FINE), FINE), :] = high[:, 256 * n : 256 * (n + 1)]
            ztable[n, pl.ds(pl.multiple_of(NZ + a * FINE, FINE), FINE), :] = low[:, 256 * n : 256 * (n + 1)]
        return carry

    lax.fori_loop(0, NZ // FINE, z_rows, 0)

    def right_copy(x, d):
        peer = right_peer(d, 1)
        return pltpu.make_async_remote_copy(
            src_ref=t2.at[x, pl.ds(pl.multiple_of(peer * YO, YO), YO), :],
            dst_ref=q.at[x, right],
            send_sem=qsend.at[x],
            recv_sem=qrecv.at[x],
            device_id=(left, peer),
            device_id_type=MESH,
        )

    def u_copy(k, p):
        peer = left_peer(p, 1)
        return pltpu.make_async_remote_copy(
            src_ref=v.at[k, pl.ds(pl.multiple_of(peer * 8, 8), 8), :],
            dst_ref=u.at[pl.ds(pl.multiple_of(left * YL + 8 * k, 8), 8), :],
            send_sem=usend,
            recv_sem=urecv,
            device_id=(peer, right),
            device_id_type=MESH,
        )

    def b_copy(n, d):
        peer = right_peer(d, 1)
        return pltpu.make_async_remote_copy(
            src_ref=t3.at[pl.ds(pl.multiple_of(peer * YO, YO), YO), pl.ds(pl.multiple_of(256 * n, 256), 256)],
            dst_ref=result.at[XA + right, :, pl.ds(pl.multiple_of(256 * n, 256), 256)],
            send_sem=bsend,
            recv_sem=brecv,
            device_id=(left, peer),
            device_id_type=MESH,
        )

    def arrived(ref, sem):
        pltpu.make_async_copy(ref, ref, sem).wait()

    def left_bytes(x, modes):
        return r1.at[pl.ds(x, modes), pl.ds(0, LEFT - 1)]

    def right_bytes(x):
        return q.at[x, pl.ds(0, RIGHT - 1)]

    def w_bytes(b):
        return w.at[pl.ds(b * RIGHT * LEFT, (RIGHT - 1) * LEFT)]

    def u_bytes():
        return u.at[pl.ds(0, NY - YL), :]

    def b_bytes():
        return result.at[pl.ds(XA, RIGHT - 1)]

    def ratio(of_xy, n):
        symbol = jnp.concatenate([of_xy, of_xy], axis=1) + sz[:, 256 * n : 256 * (n + 1)]
        return (1.0 - 0.2 * symbol) / (1.0 + 0.2 * symbol)

    def z_modes(m, n):
        both = dot(zlhs[0 : 2 * m, :], ztable[n, 0:NZ, :])
        return both[0:m] + (both[m:] + dot(zlhs[0:m, :], ztable[n, NZ : 2 * NZ, :]))

    def y_of_first(x):
        @pl.when(x == 0)
        def _():
            arrived(left_bytes(0, EARLY), lrecv.at[0])

        @pl.when(x >= EARLY)
        def _():
            arrived(left_bytes(x, 1), lrecv.at[x])

        lines = r1[x].reshape(64, 2, 8, 128)
        data = jnp.concatenate([lines[:, e].reshape(NY, 128) for e in range(2)], axis=1)
        high, low = parts(data)
        t2[x] = dot(ytable[...], jnp.concatenate([high, low, high], axis=0))
        for d in range(1, RIGHT):
            right_copy(x, d).start()
        q[x, right] = t2[x, pl.ds(pl.multiple_of(right * YO, YO), YO), :]

    def z_of_first(k):
        for e in range(2):
            x = 2 * k + e
            arrived(right_bytes(x), qrecv.at[x])
            for j in range(RIGHT):
                high, low = parts(q[x, j])
                zlhs[32 * e : 32 * (e + 1), 256 * j : 256 * (j + 1)] = high
                zlhs[64 + 32 * e : 64 + 32 * (e + 1), 256 * j : 256 * (j + 1)] = low
        of_y = sym[pl.ds(pl.multiple_of(right * YO, YO), YO), :]
        for n in range(4):
            modes = z_modes(64, n)
            for e in range(2):
                x = 2 * k + e
                result[x, :, 256 * n : 256 * (n + 1)] = modes[32 * e : 32 * (e + 1)] * ratio(
                    sx[left * XO + x] + of_y, n
                )

    def z_of_second(k):
        arrived(w_bytes(k), wrecv.at[k])
        for j in range(RIGHT):
            lines = w[pl.ds((k * RIGHT + j) * LEFT, LEFT)].reshape(LEFT, 2, 8, 128)
            for half in range(2):
                high, low = parts(lines[:, half].reshape(128, 128))
                column = 256 * j + 128 * half
                zlhs[0:128, column : column + 128] = high
                zlhs[128:256, column : column + 128] = low
        for n in range(4):
            v[k, :, 256 * n : 256 * (n + 1)] = z_modes(128, n)

        def send(p, carry):
            u_copy(k, p).start()
            return carry

        lax.fori_loop(1, LEFT, send, 0)
        u[pl.ds(pl.multiple_of(left * YL + 8 * k, 8), 8), :] = v[k, pl.ds(pl.multiple_of(left * 8, 8), 8), :]

    def y_of_second():
        arrived(u_bytes(), urecv)
        of_xy = sx[left * XO + XA + right] + sym[...]
        for n in range(4):
            high, low = parts(u[:, 256 * n : 256 * (n + 1)])
            modes = dot(ytable[...], jnp.concatenate([high, low, high], axis=0))
            t3[:, 256 * n : 256 * (n + 1)] = modes * ratio(of_xy, n)
            if n < 2:
                for d in range(1, RIGHT):
                    b_copy(n, d).start()
        result[XA + right] = t3[pl.ds(pl.multiple_of(right * YO, YO), YO), :]

    def step(i, carry):
        @pl.when(i < 4)
        def _():
            z_of_second(i)
            first = i + 1
            last = jnp.where(i < 3, i + 2, XA - EARLY)
            lax.fori_loop(first * (LEFT - 1), last * (LEFT - 1), send_left, 0)

        @pl.when(i == 4)
        def _():
            y_of_second()

        @pl.when(i >= 4)
        def _():
            z_of_first(i - 4)

        def first(x, carry):
            y_of_first(x)
            return carry

        lax.fori_loop(jnp.where(i < 2, 2 * i, jnp.minimum(i + 2, XA)), jnp.where(i < 1, 2, jnp.minimum(i + 3, XA)), first, 0)

        @pl.when((i == 4) | (i == 5))
        def _():
            for d in range(1, RIGHT):
                b_copy(i - 2, d).start()

        return carry

    lax.fori_loop(0, 8, step, 0)
    def sent_first(x, carry):
        @pl.when(x == 0)
        def _():
            arrived(left_bytes(0, EARLY), lsend.at[0])

        @pl.when(x >= EARLY)
        def _():
            arrived(left_bytes(x, 1), lsend.at[x])

        arrived(right_bytes(x), qsend.at[x])
        return carry

    def sent_second(p, carry):
        arrived(w_bytes(p), wsend.at[p])
        return carry

    lax.fori_loop(0, XA, sent_first, 0)
    lax.fori_loop(0, 4, sent_second, 0)
    arrived(u_bytes(), usend)
    arrived(b_bytes(), brecv)
    arrived(b_bytes(), bsend)


def body(signal, symbol_x, symbol_y, symbol_z):
    coarse, fine = factor_tables(NZ)
    xtable = split_table(NX, x_order())
    ytable = split_table(NY, np.arange(KY))
    dma = pltpu.SemaphoreType.DMA
    any_space = pl.BlockSpec(memory_space=pl.ANY)
    vmem = pl.BlockSpec(memory_space=pltpu.VMEM)
    return pl.pallas_call(
        kernel,
        out_shape=pltpu.VMEM((XO, YO, KZ), F32),
        in_specs=[any_space] * 8,
        out_specs=vmem,
        scratch_shapes=[
            pltpu.VMEM((8, NX, 8, 128), F32),
            pltpu.VMEM(xtable.shape, BF16),
            pltpu.VMEM(ytable.shape, BF16),
            pltpu.VMEM(coarse.shape, F32),
            pltpu.VMEM(fine.shape, F32),
            pltpu.VMEM((4, 2 * NZ, 256), BF16),
            pltpu.VMEM((KX, PITCH, 128), F32),
            pltpu.VMEM((XA, LEFT, 64, 128), F32),
            pltpu.VMEM((XA, KY, ZL), F32),
            pltpu.VMEM((XA, RIGHT, YO, ZL), F32),
            pltpu.VMEM((4 * RIGHT * LEFT, 16, 128), F32),
            pltpu.VMEM((4, 8 * LEFT, KZ), F32),
            pltpu.VMEM((NY, KZ), F32),
            pltpu.VMEM((KY, KZ), F32),
            pltpu.VMEM((256, NZ), BF16),
            pltpu.VMEM((KY, 128), F32),
            pltpu.SMEM((NX,), F32),
            pltpu.VMEM((1, NY), F32),
            pltpu.VMEM((1, NZ), F32),
            pltpu.SemaphoreType.REGULAR,
            dma((8,)),
            dma((7,)),
            dma((XA,)),
            dma((XA,)),
            dma((XA,)),
            dma((XA,)),
            dma((4,)),
            dma((4,)),
            dma(()),
            dma(()),
            dma(()),
            dma(()),
        ],
        compiler_params=pltpu.CompilerParams(
            collective_id=0, has_side_effects=True, vmem_limit_bytes=58 * 2**20
        ),
    )(
        signal,
        jnp.asarray(xtable),
        jnp.asarray(ytable),
        jnp.asarray(coarse),
        jnp.asarray(fine),
        symbol_x,
        symbol_y.reshape(1, NY),
        symbol_z.reshape(1, NZ),
    )


def solution(mesh):
    in_specs = (P(None, "left", "right"), P(), P(), P())
    out_specs = P("left", "right", None)
    return jax.shard_map(body, mesh=mesh, in_specs=in_specs, out_specs=out_specs, check_vma=False)
```
